32 devices in a mesh: section: 2 (over y), tensor: 16 (over z, x, core).
Axes of the slice: x: 2, y: 2, z: 4, core: 2. Of those that a mesh axis runs over, the one named last changes fastest.
Arguments:
- embedded: bfloat16 [32, 6144], P(None, 'tensor'), may hold values from -6 to 6
- norm_gain: float32 [2, 6144], P('section'), may hold values from 0.25 to 1.75
- qkv_weight: bfloat16 [2, 6144, 3, 4096], P('section', None, None, 'tensor'), may hold values from -0.078125 to 0.078125
- out_weight: bfloat16 [2, 4096, 6144], P('section', 'tensor'), may hold values from -0.09375 to 0.09375
- cache_keys: bfloat16 [2, 32, 256, 4096], P('section', None, None, 'tensor'), may hold values from -6 to 6
- cache_values: bfloat16 [2, 32, 256, 4096], P('section', None, None, 'tensor'), may hold values from -6 to 6
- dwa_weights: float32 [3, 4], replicated, may hold values from 0.05 to 0.45
- dwa_sources: int32 [3, 4], replicated, may hold values from 0 to 2, as said below
- token_order: int32 [32], replicated, may hold values from 0 to 31, each once
- kv_lengths: int32 [32], replicated, may hold values from 1 to 256, as said below
Outputs:
- final_mix: bfloat16 [32, 6144], P('section', 'tensor')
The draws below stay inside these ranges and needn't reach their ends.
Inputs may be any that keep to these rules, and one draw needn't show every extreme that they name: `dwa_sources`: each entry of row i lies in 0 to i, and the first entry of row i is i. `token_order`: a permutation of 0 to 31. `kv_lengths`: some token sees all 256 positions.
All inputs are finite; a program needn't handle non-finite values.
Results may differ from the reference program's by a relative error of at most 0.025.
Values may be sent and summed in bfloat16 or wider, within the bound.
A program may use at most 128 MiB of HBM per device.

```python
import jax
import jax.numpy as jnp
from jax import lax

D = 6144
HD = 128
HEADS = 32
SLOTS = 4
BATCH = 32
CACHE = 256
LAYERS = 2
N_TENSOR = 16


def draw_dwa_sources(key, part):
    row_index = jnp.arange(LAYERS + 1, dtype=jnp.int32)[:, None]
    raw_draw = jax.random.randint(key, (LAYERS + 1, SLOTS), 0, 1 << 20, dtype=jnp.int32)
    picked = raw_draw % (row_index + 1)
    first_slot = jnp.arange(SLOTS, dtype=jnp.int32)[None, :] == 0
    return jnp.where(first_slot, row_index, picked).astype(jnp.int32)


def draw_kv_lengths(key, part):
    key_spread = jax.random.fold_in(key, 11)
    key_chosen = jax.random.fold_in(key, 12)
    spread = jax.random.randint(key_spread, (BATCH,), 1, CACHE + 1, dtype=jnp.int32)
    chosen = jax.random.randint(key_chosen, (), 0, BATCH, dtype=jnp.int32)
    return jnp.where(jnp.arange(BATCH, dtype=jnp.int32) == chosen, CACHE, spread).astype(jnp.int32)


def block_scale(stream_key, shape, split, smallest, largest):
    def one(position, blocks):
        heights = jax.random.uniform(jax.random.fold_in(jax.random.fold_in(stream_key, 6), position), (blocks,), jnp.float32, smallest / len(split), largest / len(split))
        return jnp.repeat(jnp.exp(heights), shape[position] // blocks).reshape((-1,) + (1,) * (len(shape) - position - 1))

    gain = one(*split[0])
    for cut in split[1:]:
        gain = gain * one(*cut)
    return gain


def scatter_about(own_key, dims, scale, reach, shards=(), kind=jnp.bfloat16):
    level = block_scale(own_key, dims, shards, -0.22, 0.18) if shards else 1.0
    drawn = jax.random.normal(own_key, dims, jnp.float32) * scale * level
    return jnp.minimum(jnp.maximum(drawn, -reach), reach).astype(kind)


def setup_inputs(seed: int = 0) -> dict:
    seeds = jax.random.split(jax.random.key(seed), 11)
    embedded = scatter_about(seeds[0], (BATCH, D), 1.0, 6.0, ((1, 16),))
    norm_gain = jnp.clip(1.0 + 0.15 * jax.random.normal(seeds[1], (LAYERS, D), jnp.float32), 0.25, 1.75)
    qkv_weight = scatter_about(seeds[2], (LAYERS, D, 3, HEADS * HD), D ** -0.5, 0.078125, ((0, 2), (3, 16)))
    out_weight = scatter_about(seeds[3], (LAYERS, HEADS * HD, D), (HEADS * HD) ** -0.5, 0.09375, ((0, 2), (1, 16)))
    cache_keys = scatter_about(seeds[4], (LAYERS, BATCH, CACHE, HEADS * HD), 1.0, 6.0, ((0, 2), (3, 16)))
    cache_values = scatter_about(seeds[5], (LAYERS, BATCH, CACHE, HEADS * HD), 1.0, 6.0, ((0, 2), (3, 16)))
    dwa_weights = jnp.clip(jax.random.uniform(seeds[6], (LAYERS + 1, SLOTS), jnp.float32, 0.05, 0.45), 0.05, 0.45)
    dwa_sources = draw_dwa_sources(jax.random.fold_in(seeds[10], 71), 0)
    token_order = jax.random.permutation(seeds[8], BATCH).astype(jnp.int32)
    kv_lengths = draw_kv_lengths(jax.random.fold_in(seeds[10], 71), 0)
    return {"embedded": embedded, "norm_gain": norm_gain, "qkv_weight": qkv_weight, "out_weight": out_weight, "cache_keys": cache_keys, "cache_values": cache_values, "dwa_weights": dwa_weights, "dwa_sources": dwa_sources, "token_order": token_order, "kv_lengths": kv_lengths}


def coefficients(dwa_weights, dwa_sources, count):
    levels = jnp.arange(count, dtype=jnp.int32)
    matches = (dwa_sources[:, :, None] == levels[None, None, :]).astype(jnp.float32)
    return lax.optimization_barrier(jnp.sum(dwa_weights[:, :, None] * matches, axis=1))

def attend(normed, qkv_local, key_rows, value_rows, lengths):
    row_count = normed.shape[0]
    heads_here = qkv_local.shape[-1] // HD
    projected = jnp.dot(normed, qkv_local.reshape(normed.shape[1], -1), preferred_element_type=jnp.float32)
    projected = projected.reshape(row_count, 3, heads_here, HD)
    query_rows = (projected[:, 0] * HD ** (-0.5)).astype(jnp.bfloat16)
    key_new = projected[:, 1].astype(jnp.bfloat16)
    value_new = projected[:, 2].astype(jnp.bfloat16)
    cache_len = key_rows.shape[1]
    key_rows = key_rows.reshape(row_count, cache_len, heads_here, HD)
    value_rows = value_rows.reshape(row_count, cache_len, heads_here, HD)
    scores = jnp.einsum('bhd,bchd->bhc', query_rows.astype(jnp.float32), key_rows.astype(jnp.float32))
    own_score = lax.optimization_barrier(jnp.sum(query_rows.astype(jnp.float32) * key_new.astype(jnp.float32), axis=-1))
    visible = jnp.arange(cache_len, dtype=jnp.int32)[None, None, :] < lengths[:, None, None]
    weights = jnp.where(visible, jnp.exp(scores), 0.0)
    own_weight = jnp.exp(own_score)
    denominator = lax.optimization_barrier(jnp.sum(weights, axis=-1)) + own_weight
    attended = jnp.einsum('bhc,bchd->bhd', weights.astype(jnp.bfloat16).astype(jnp.float32), value_rows.astype(jnp.float32))
    attended = attended + own_weight.astype(jnp.bfloat16).astype(jnp.float32)[:, :, None] * value_new.astype(jnp.float32)
    return (attended / denominator[:, :, None]).astype(jnp.bfloat16).reshape(row_count, heads_here * HD)

def head_projection(attended, weight):
    row_count = attended.shape[0]
    group = attended.shape[1] // N_TENSOR
    grouped_rows = jnp.transpose(attended.reshape(row_count, N_TENSOR, group), (1, 0, 2))
    grouped_weights = weight.reshape(N_TENSOR, group, weight.shape[1])

    def one_group(pair):
        rows, block = pair
        return jnp.dot(rows, block, preferred_element_type=jnp.float32).astype(jnp.bfloat16)
    parts = lax.map(one_group, (grouped_rows, grouped_weights))
    parts = lax.optimization_barrier(parts)
    return lax.optimization_barrier(jnp.sum(parts.astype(jnp.float32), axis=0))

def reference(embedded, norm_gain, qkv_weight, out_weight, cache_keys, cache_values, dwa_weights, dwa_sources, token_order, kv_lengths):
    coef_table = coefficients(dwa_weights, dwa_sources, LAYERS + 1)
    outputs = [embedded]
    for level_index in range(LAYERS):
        stacked = jnp.stack(outputs).astype(jnp.float32)
        averaged = jnp.tensordot(coef_table[level_index, :len(outputs)], stacked, axes=1, precision=lax.Precision.HIGHEST).astype(jnp.bfloat16)
        floats = averaged.astype(jnp.float32)
        inv_rms = lax.rsqrt(lax.optimization_barrier(jnp.mean(floats * floats, axis=-1, keepdims=True)) + 1e-05)
        normed = (floats * inv_rms * norm_gain[level_index][None, :]).astype(jnp.bfloat16)
        key_rows = jnp.take(cache_keys[level_index], token_order, axis=0)
        value_rows = jnp.take(cache_values[level_index], token_order, axis=0)
        attended = attend(normed, qkv_weight[level_index], key_rows, value_rows, kv_lengths)
        projected = head_projection(attended, out_weight[level_index])
        outputs.append((floats + projected).astype(jnp.bfloat16))
    stacked = jnp.stack(outputs).astype(jnp.float32)
    final_mix = jnp.tensordot(coef_table[LAYERS], stacked, axes=1, precision=lax.Precision.HIGHEST)
    return final_mix.astype(jnp.bfloat16)
```

```python
import functools

import jax
import jax.numpy as jnp
from jax import lax
from jax.experimental import pallas as pl
from jax.experimental.pallas import tpu as pltpu
from jax.sharding import PartitionSpec as P

HD = 128
SUB = 8
MESH = pl.DeviceIdType.MESH
F32 = jnp.float32
BF16 = jnp.bfloat16


def kernel(
    sections,
    tensors,
    emb_ref,
    gain_ref,
    w_hbm,
    wo_hbm,
    k_hbm,
    v_hbm,
    dw_ref,
    ds_ref,
    order_ref,
    len_ref,
    out_ref,
    w_ref,
    wo_ref,
    k_ref,
    v_ref,
    g_ref,
    fin_ref,
    acc_ref,
    x_ref,
    q_ref,
    s_ref,
    p_ref,
    d_ref,
    o_ref,
    part_ref,
    pair_ref,
    ps_ref,
    rs_ref,
    outb_ref,
    mix_ref,
    loc_sem,
    g_recv,
    g_send,
    fwd_send,
    pair_send,
    pair_recv,
    rs_send,
    rs_recv,
    bc_send,
    fin_send,
    fin_recv,
):
    chips = tensors // 2
    s = lax.axis_index("section")
    t = lax.axis_index("tensor")
    c = lax.rem(t, 2)
    m0 = t // 2
    partner = (s, t + 1 - 2 * c)
    rows, feats = emb_ref.shape
    slots = dw_ref.shape[1]
    width = w_ref.shape[2]
    heads = width // HD

    def coef(i, j):
        total = jnp.float32(0.0)
        for k in range(slots):
            total = total + jnp.where(ds_ref[i, k] == j, dw_ref[i, k], jnp.float32(0.0))
        return total

    w_copies = [
        pltpu.make_async_copy(w_hbm.at[j], w_ref.at[j], loc_sem.at[j]) for j in range(3)
    ]
    k_copy = pltpu.make_async_copy(k_hbm, k_ref, loc_sem.at[3])
    v_copy = pltpu.make_async_copy(v_hbm, v_ref, loc_sem.at[4])
    wo_copy = pltpu.make_async_copy(wo_hbm, wo_ref, loc_sem.at[5])
    for cp in w_copies + [k_copy, v_copy, wo_copy]:
        cp.start()

    barrier = pltpu.get_barrier_semaphore()
    for j in range(sections):
        for m in range(chips):

            @pl.when(jnp.logical_or(s != j, m0 != m))
            def _():
                pl.semaphore_signal(
                    barrier, inc=1, device_id=(jnp.int32(j), 2 * m + c), device_id_type=MESH
                )

    pl.semaphore_signal(barrier, inc=1, device_id=partner, device_id_type=MESH)
    pl.semaphore_wait(barrier, sections * chips)

    def own_copy(m):
        return pltpu.make_async_remote_copy(
            src_ref=emb_ref,
            dst_ref=g_ref.at[0, c, m0],
            send_sem=g_send.at[m],
            recv_sem=g_recv.at[0, c, m0],
            device_id=(s, 2 * m + c),
            device_id_type=MESH,
        )

    def partner_copy(src, level, m):
        return pltpu.make_async_remote_copy(
            src_ref=src,
            dst_ref=g_ref.at[level, c, m],
            send_sem=fwd_send.at[level, m],
            recv_sem=g_recv.at[level, c, m],
            device_id=partner,
            device_id_type=MESH,
        )

    def arrive(level, parity, m):
        pltpu.make_async_copy(
            g_ref.at[level, parity, m], g_ref.at[level, parity, m], g_recv.at[level, parity, m]
        ).wait()

    for k in range(1, chips):
        own_copy(lax.rem(m0 + k, chips)).start()
    partner_copy(emb_ref, 0, m0).start()
    g_ref[0, c, m0] = emb_ref[...]
    for k in range(1, chips):
        m = lax.rem(m0 + k, chips)
        arrive(0, c, m)
        partner_copy(g_ref.at[0, c, m], 0, m).start()
    for m in range(chips):
        arrive(0, 1 - c, m)

    cf = coef(s, 0)
    mix_ref[...] = cf * emb_ref[...].astype(F32)
    for tt in range(tensors):
        acc_ref[:, tt * feats : (tt + 1) * feats] = cf * g_ref[0, tt % 2, tt // 2].astype(F32)

    def add_level(level, carry):
        for m in range(chips):
            arrive(level, c, m)
            partner_copy(g_ref.at[level, c, m], level, m).start()
        for m in range(chips):
            arrive(level, 1 - c, m)
        cl = coef(s, level)
        mix_ref[...] = mix_ref[...] + cl * g_ref[level, c, m0].astype(F32)
        for tt in range(tensors):
            cols = slice(tt * feats, (tt + 1) * feats)
            acc_ref[:, cols] = acc_ref[:, cols] + cl * g_ref[level, tt % 2, tt // 2].astype(F32)
        return carry

    lax.fori_loop(1, s + 1, add_level, 0)

    squares = jnp.zeros((rows, HD), F32)
    for tt in range(tensors * feats // HD):
        cols = slice(tt * HD, (tt + 1) * HD)
        avg = acc_ref[:, cols].astype(BF16).astype(F32)
        acc_ref[:, cols] = avg
        squares = squares + avg * avg
        x_ref[:, cols] = (avg * gain_ref[:, cols]).astype(BF16)
    model = tensors * feats
    inv_rms = lax.rsqrt(jnp.sum(squares, axis=1, keepdims=True) / model + 1e-05)

    x = x_ref[...]
    w_copies[0].wait()
    query = (jnp.dot(x, w_ref[0], preferred_element_type=F32) * inv_rms * HD ** (-0.5)).astype(BF16)
    query = query.astype(F32)
    q_ref[...] = query
    w_copies[1].wait()
    key_new = (jnp.dot(x, w_ref[1], preferred_element_type=F32) * inv_rms).astype(BF16).astype(F32)
    w_copies[2].wait()
    value_new = (jnp.dot(x, w_ref[2], preferred_element_type=F32) * inv_rms).astype(BF16).astype(F32)

    cache = k_ref.shape[1]
    head_of_lane = lax.broadcasted_iota(jnp.int32, (SUB, width), 1) // HD
    head_rows = lax.broadcasted_iota(jnp.int32, (SUB, width), 0)
    head_mask = head_of_lane == head_rows
    position = lax.broadcasted_iota(jnp.int32, (SUB, cache), 1)
    group = 8

    k_copy.wait()

    def score_step(step, carry):
        for u in range(group):
            b = step * group + u
            row = order_ref[b]
            qb = jnp.broadcast_to(q_ref[pl.ds(b, 1), :], (SUB, width))
            qb = jnp.where(head_mask, qb, 0.0).astype(BF16)
            sc = lax.dot_general(
                qb, k_ref[row], (((1,), (1,)), ((), ())), preferred_element_type=F32
            )
            s_ref[pl.ds(pl.multiple_of(b * SUB, SUB), SUB), :] = jnp.where(
                position < len_ref[b], sc, -1e30
            )
        return carry

    lax.fori_loop(0, rows // group, score_step, 0)
    p = jnp.exp(s_ref[...])
    d_ref[...] = jnp.broadcast_to(jnp.sum(p, axis=1, keepdims=True), (rows * SUB, HD))
    p_ref[...] = p.astype(BF16).reshape(rows, SUB, cache)

    v_copy.wait()

    def value_step(step, carry):
        for u in range(group):
            b = step * group + u
            row = order_ref[b]
            pv = jnp.dot(p_ref[b], v_ref[row], preferred_element_type=F32)
            for h in range(heads):
                o_ref[h, pl.ds(pl.multiple_of(b * SUB, SUB), SUB), :] = pv[
                    :, h * HD : (h + 1) * HD
                ]
        return carry

    lax.fori_loop(0, rows // group, value_step, 0)

    pieces = []
    for h in range(heads):
        lanes = slice(h * HD, (h + 1) * HD)
        own = jnp.exp(jnp.sum(query[:, lanes] * key_new[:, lanes], axis=1, keepdims=True))
        total = o_ref[h, pl.ds(h, rows, stride=SUB), :]
        total = total + own.astype(BF16).astype(F32) * value_new[:, lanes]
        den = d_ref[pl.ds(h, rows, stride=SUB), :] + own
        pieces.append((total / den).astype(BF16))
    attended = jnp.concatenate(pieces, axis=1)

    def pair_copy(m):
        return pltpu.make_async_remote_copy(
            src_ref=part_ref.at[1 - c, m],
            dst_ref=pair_ref.at[m],
            send_sem=pair_send.at[m],
            recv_sem=pair_recv.at[m],
            device_id=partner,
            device_id_type=MESH,
        )

    def rs_copy(m):
        return pltpu.make_async_remote_copy(
            src_ref=ps_ref.at[m],
            dst_ref=rs_ref.at[m0],
            send_sem=rs_send.at[m],
            recv_sem=rs_recv.at[m0],
            device_id=(s, 2 * m + c),
            device_id_type=MESH,
        )

    wo_copy.wait()
    for m in range(chips):
        both = jnp.dot(
            attended,
            wo_ref[:, 2 * m * feats : 2 * (m + 1) * feats],
            preferred_element_type=F32,
        ).astype(BF16)
        part_ref[0, m] = both[:, :feats]
        part_ref[1, m] = both[:, feats:]
        pair_copy(m).start()
    for m in range(chips):
        pair_copy(m).wait_recv()
        ps_ref[m] = (part_ref[c, m].astype(F32) + pair_ref[m].astype(F32)).astype(BF16)

        @pl.when(m0 != m)
        def _():
            rs_copy(m).start()

    produced = mix_ref[...].astype(BF16).astype(F32) + ps_ref[m0].astype(F32)
    for k in range(1, chips):
        m = lax.rem(m0 + k, chips)
        pltpu.make_async_copy(rs_ref.at[m], rs_ref.at[m], rs_recv.at[m]).wait()
        produced = produced + rs_ref[m].astype(F32)
    outb_ref[...] = produced.astype(BF16)

    def bc_copy(j, m):
        return pltpu.make_async_remote_copy(
            src_ref=outb_ref,
            dst_ref=g_ref.at[s + 1, c, m0],
            send_sem=bc_send.at[j, m],
            recv_sem=g_recv.at[s + 1, c, m0],
            device_id=(j, 2 * m + c),
            device_id_type=MESH,
        )

    def fin_copy(j):
        return pltpu.make_async_remote_copy(
            src_ref=outb_ref,
            dst_ref=fin_ref.at[s],
            send_sem=fin_send.at[j],
            recv_sem=fin_recv.at[s],
            device_id=(j, t),
            device_id_type=MESH,
        )

    def send_later(j, carry):
        for m in range(chips):
            bc_copy(j, m).start()
        return carry

    def send_earlier(j, carry):
        fin_copy(j).start()
        return carry

    lax.fori_loop(s + 1, sections, send_later, 0)
    lax.fori_loop(0, s, send_earlier, 0)

    mix_ref[...] = coef(sections, 0) * emb_ref[...].astype(F32)

    def mix_before(level, carry):
        mix_ref[...] = mix_ref[...] + coef(sections, level) * g_ref[level, c, m0].astype(F32)
        return carry

    lax.fori_loop(1, s + 1, mix_before, 0)
    mix_ref[...] = mix_ref[...] + coef(sections, s + 1) * outb_ref[...].astype(F32)

    def mix_after(j, carry):
        pltpu.make_async_copy(fin_ref.at[j], fin_ref.at[j], fin_recv.at[j]).wait()
        mix_ref[...] = mix_ref[...] + coef(sections, j + 1) * fin_ref[j].astype(F32)
        return carry

    lax.fori_loop(s + 1, sections, mix_after, 0)
    out_rows = out_ref.shape[0]
    for j in range(sections):

        @pl.when(s == j)
        def _():
            out_ref[...] = mix_ref[j * out_rows : (j + 1) * out_rows, :].astype(BF16)

    for k in range(1, chips):
        own_copy(lax.rem(m0 + k, chips)).wait_send()
    for m in range(chips):
        partner_copy(emb_ref, 0, m).wait_send()
        pair_copy(m).wait_send()

        @pl.when(m0 != m)
        def _():
            rs_copy(m).wait_send()

    def drain_forward(level, carry):
        for m in range(chips):
            partner_copy(emb_ref, level, m).wait_send()
        return carry

    def drain_later(j, carry):
        for m in range(chips):
            bc_copy(j, m).wait_send()
        return carry

    def drain_earlier(j, carry):
        fin_copy(j).wait_send()
        return carry

    lax.fori_loop(1, s + 1, drain_forward, 0)
    lax.fori_loop(s + 1, sections, drain_later, 0)
    lax.fori_loop(0, s, drain_earlier, 0)


def per_device(sections, tensors, emb, gain, qkv, wo, ck, cv, dw, ds, order, lengths):
    rows, feats = emb.shape
    model = feats * tensors
    chips = tensors // 2
    w = jnp.transpose(qkv, (0, 2, 1, 3))[0]
    width = w.shape[-1]
    cache = ck.shape[2]
    vmem = pl.BlockSpec(memory_space=pltpu.VMEM)
    smem = pl.BlockSpec(memory_space=pltpu.SMEM)
    hbm = pl.BlockSpec(memory_space=pl.ANY)
    dma = pltpu.SemaphoreType.DMA
    return pl.pallas_call(
        functools.partial(kernel, sections, tensors),
        out_shape=jax.ShapeDtypeStruct((rows // sections, feats), BF16),
        in_specs=[vmem, vmem, hbm, hbm, hbm, hbm, smem, smem, smem, smem],
        out_specs=vmem,
        scratch_shapes=[
            pltpu.VMEM(w.shape, BF16),
            pltpu.VMEM(wo.shape[1:], BF16),
            pltpu.VMEM(ck.shape[1:], BF16),
            pltpu.VMEM(cv.shape[1:], BF16),
            pltpu.VMEM((sections, 2, chips, rows, feats), BF16),
            pltpu.VMEM((sections, rows, feats), BF16),
            pltpu.VMEM((rows, model), F32),
            pltpu.VMEM((rows, model), BF16),
            pltpu.VMEM((rows, width), F32),
            pltpu.VMEM((rows * SUB, cache), F32),
            pltpu.VMEM((rows, SUB, cache), BF16),
            pltpu.VMEM((rows * SUB, HD), F32),
            pltpu.VMEM((width // HD, rows * SUB, HD), F32),
            pltpu.VMEM((2, chips, rows, feats), BF16),
            pltpu.VMEM((chips, rows, feats), BF16),
            pltpu.VMEM((chips, rows, feats), BF16),
            pltpu.VMEM((chips, rows, feats), BF16),
            pltpu.VMEM((rows, feats), BF16),
            pltpu.VMEM((rows, feats), F32),
            dma((6,)),
            dma((sections, 2, chips)),
            dma((chips,)),
            dma((sections, chips)),
            dma((chips,)),
            dma((chips,)),
            dma((chips,)),
            dma((chips,)),
            dma((sections, chips)),
            dma((sections,)),
            dma((sections,)),
        ],
        compiler_params=pltpu.CompilerParams(
            collective_id=0, has_side_effects=True, vmem_limit_bytes=56 * 1024 * 1024
        ),
    )(emb, gain, w, wo[0], ck[0], cv[0], dw, ds, order, lengths)


def solution(mesh):
    placed = (
        P(None, "tensor"),
        P("section", None),
        P("section", None, None, "tensor"),
        P("section", "tensor", None),
        P("section", None, None, "tensor"),
        P("section", None, None, "tensor"),
        P(),
        P(),
        P(),
        P(),
    )
    return jax.shard_map(
        functools.partial(per_device, mesh.shape["section"], mesh.shape["tensor"]),
        mesh=mesh,
        in_specs=placed,
        out_specs=P("section", "tensor"),
        check_vma=False,
    )
```

```python
import functools

import jax
import jax.numpy as jnp
from jax import lax
from jax.experimental import pallas as pl
from jax.experimental.pallas import tpu as pltpu
from jax.sharding import PartitionSpec as P

HD = 128
SUB = 8
MESH = pl.DeviceIdType.MESH
F32 = jnp.float32
BF16 = jnp.bfloat16


def kernel(
    sections,
    tensors,
    emb_ref,
    gain_ref,
    w_hbm,
    wo_hbm,
    k_hbm,
    v_hbm,
    dw_ref,
    ds_ref,
    order_ref,
    len_ref,
    out_ref,
    w_ref,
    wo_ref,
    k_ref,
    v_ref,
    g_ref,
    fin_ref,
    acc_ref,
    x_ref,
    q_ref,
    s_ref,
    p_ref,
    d_ref,
    o_ref,
    part_ref,
    pair_ref,
    ps_ref,
    rs_ref,
    fps_ref,
    frs_ref,
    outb_ref,
    mix_ref,
    avl_ref,
    loc_sem,
    g_recv,
    g_send,
    fwd_send,
    pair_send,
    pair_recv,
    rs_send,
    rs_recv,
    frs_send,
    frs_recv,
    bc_send,
    fin_send,
    fin_recv,
    ready_sem,
):
    chips = tensors // 2
    last = sections - 1
    s = lax.axis_index("section")
    t = lax.axis_index("tensor")
    c = lax.rem(t, 2)
    m0 = t // 2
    partner = (s, t + 1 - 2 * c)
    rows, feats = emb_ref.shape
    slots = dw_ref.shape[1]
    width = w_ref.shape[3]
    heads = width // HD

    def coef(i, j):
        total = jnp.float32(0.0)
        for k in range(slots):
            total = total + jnp.where(ds_ref[i, k] == j, dw_ref[i, k], jnp.float32(0.0))
        return total

    def remote(src, dst, send, recv, device):
        return pltpu.make_async_remote_copy(
            src_ref=src,
            dst_ref=dst,
            send_sem=send,
            recv_sem=recv,
            device_id=device,
            device_id_type=MESH,
        )

    def landed(ref, sem):
        pltpu.make_async_copy(ref, ref, sem).wait()

    barrier = pltpu.get_barrier_semaphore()
    pl.semaphore_signal(barrier, inc=1, device_id=partner, device_id_type=MESH)
    for k in range(1, chips):
        m = lax.rem(m0 + k, chips)
        pl.semaphore_signal(barrier, inc=1, device_id=(s, 2 * m + c), device_id_type=MESH)
    for k in range(1, sections):
        j = lax.rem(s + k, sections)
        pl.semaphore_signal(barrier, inc=1, device_id=(j, t), device_id_type=MESH)

    w_copies = [
        pltpu.make_async_copy(w_hbm.at[j], w_ref.at[j], loc_sem.at[j]) for j in range(3)
    ]
    k_copy = pltpu.make_async_copy(k_hbm, k_ref, loc_sem.at[3])
    v_copy = pltpu.make_async_copy(v_hbm, v_ref, loc_sem.at[4])
    wo_copy = pltpu.make_async_copy(wo_hbm, wo_ref, loc_sem.at[5])
    for cp in w_copies + [k_copy, v_copy, wo_copy]:
        cp.start()
    acc_ref[...] = jnp.zeros_like(acc_ref)

    pl.semaphore_wait(barrier, chips + sections - 1)
    for k in range(1, sections):
        j = lax.rem(s + k, sections)
        pl.semaphore_signal(ready_sem, inc=1, device_id=(j, t), device_id_type=MESH)

    def spread(src, level, group, m):
        return remote(
            src,
            g_ref.at[level, c, m0],
            g_send.at[group, m],
            g_recv.at[level, c, m0],
            (s, 2 * m + c),
        )

    def forward(src, level, m):
        return remote(
            src, g_ref.at[level, c, m], fwd_send.at[level, m], g_recv.at[level, c, m], partner
        )

    def arrive(level, parity, m):
        landed(g_ref.at[level, parity, m], g_recv.at[level, parity, m])

    def spread_start(src, level, group):
        for k in range(1, chips):
            spread(src, level, group, lax.rem(m0 + k, chips)).start()
        forward(src, level, m0).start()
        g_ref[level, c, m0] = src[...]

    def to_later(j, m):
        return remote(
            outb_ref,
            g_ref.at[s, c, m0],
            bc_send.at[j, m],
            g_recv.at[s, c, m0],
            (j, 2 * m + c),
        )

    def to_earlier(j):
        return remote(outb_ref, fin_ref.at[s], fin_send.at[j], fin_recv.at[s], (j, t))

    @pl.when(s == 0)
    def _():
        outb_ref[...] = emb_ref[...]

    @pl.when(s > 0)
    def _():
        spread_start(emb_ref, 0, 0)

        def add_level(level, carry):
            for k in range(chips):
                m = lax.rem(m0 + k, chips)
                if k == 0:

                    @pl.when(level > 0)
                    def _():
                        arrive(level, c, m)
                        forward(g_ref.at[level, c, m], level, m).start()
                else:
                    arrive(level, c, m)
                    forward(g_ref.at[level, c, m], level, m).start()
            for m in range(chips):
                arrive(level, 1 - c, m)
            cl = coef(s, level)
            for m in range(chips):
                for par in range(2):
                    acc_ref[par, m] = acc_ref[par, m] + cl * g_ref[level, par, m].astype(F32)
            return carry

        lax.fori_loop(0, s, add_level, 0)

        mix_ref[...] = jnp.zeros_like(mix_ref)

        def add_below(level, carry):
            mix_ref[...] = mix_ref[...] + coef(s - 1, level) * g_ref[level, c, m0].astype(F32)
            return carry

        lax.fori_loop(0, s, add_below, 0)
        produced = mix_ref[...].astype(BF16).astype(F32)
        for k in range(chips):
            m = lax.rem(m0 + k, chips)
            landed(rs_ref.at[m], rs_recv.at[m])
            produced = produced + rs_ref[m].astype(F32)
        outb_ref[...] = produced.astype(BF16)

    spread_start(outb_ref, s, 1)
    pl.semaphore_wait(ready_sem, sections - 1)

    @pl.when(s > 0)
    def _():
        def send_later(j, carry):
            for m in range(chips):
                to_later(j, m).start()
            return carry

        def send_earlier(j, carry):
            to_earlier(j).start()
            return carry

        lax.fori_loop(s + 1, sections, send_later, 0)
        lax.fori_loop(0, s, send_earlier, 0)

    top = coef(s, s)
    squares = jnp.zeros((rows, 1), F32)
    proj = [jnp.zeros((rows, width), F32) for _ in range(3)]
    lag = 2
    for k in range(chips + lag):
        if 0 < k < chips:
            m = lax.rem(m0 + k, chips)
            arrive(s, c, m)
            forward(g_ref.at[s, c, m], s, m).start()
        k = k - lag
        if k < 0:
            continue
        m = lax.rem(m0 + k, chips)
        arrive(s, 1 - c, m)
        gains = gain_ref[:, pl.ds(pl.multiple_of(m * 2 * feats, HD), 2 * feats)]
        for par in range(2):
            cols = slice(par * feats, (par + 1) * feats)
            avg = acc_ref[par, m] + top * g_ref[s, par, m].astype(F32)
            avg = avg.astype(BF16).astype(F32)
            squares = squares + jnp.sum(avg * avg, axis=1, keepdims=True)
            x_ref[k, :, cols] = (avg * gains[:, cols]).astype(BF16)
        if k == 0:
            for cp in w_copies:
                cp.wait()
        x = x_ref[k]
        for j in range(3):
            proj[j] = proj[j] + jnp.dot(x, w_ref[j, m], preferred_element_type=F32)
    inv_rms = lax.rsqrt(squares / (tensors * feats) + 1e-05)
    query = (proj[0] * inv_rms * HD ** (-0.5)).astype(BF16).astype(F32)
    q_ref[...] = query
    key_new = (proj[1] * inv_rms).astype(BF16).astype(F32)
    value_new = (proj[2] * inv_rms).astype(BF16).astype(F32)

    cache = k_ref.shape[1]
    head_of_lane = lax.broadcasted_iota(jnp.int32, (SUB, width), 1) // HD
    head_rows = lax.broadcasted_iota(jnp.int32, (SUB, width), 0)
    head_mask = head_of_lane == head_rows
    position = lax.broadcasted_iota(jnp.int32, (SUB, cache), 1)
    group = 8

    k_copy.wait()

    def score_step(step, carry):
        for u in range(group):
            b = step * group + u
            row = order_ref[b]
            qb = jnp.broadcast_to(q_ref[pl.ds(b, 1), :], (SUB, width))
            qb = jnp.where(head_mask, qb, 0.0).astype(BF16)
            sc = lax.dot_general(
                qb, k_ref[row], (((1,), (1,)), ((), ())), preferred_element_type=F32
            )
            s_ref[pl.ds(pl.multiple_of(b * SUB, SUB), SUB), :] = jnp.where(
                position < len_ref[b], sc, -1e30
            )
        return carry

    lax.fori_loop(0, rows // group, score_step, 0)
    p = jnp.exp(s_ref[...])
    d_ref[...] = jnp.broadcast_to(jnp.sum(p, axis=1, keepdims=True), (rows * SUB, HD))
    p_ref[...] = p.astype(BF16).reshape(rows, SUB, cache)

    v_copy.wait()

    def value_step(step, carry):
        for u in range(group):
            b = step * group + u
            row = order_ref[b]
            pv = jnp.dot(p_ref[b], v_ref[row], preferred_element_type=F32)
            for h in range(heads):
                o_ref[h, pl.ds(pl.multiple_of(b * SUB, SUB), SUB), :] = pv[
                    :, h * HD : (h + 1) * HD
                ]
        return carry

    lax.fori_loop(0, rows // group, value_step, 0)

    pieces = []
    for h in range(heads):
        lanes = slice(h * HD, (h + 1) * HD)
        own = jnp.exp(jnp.sum(query[:, lanes] * key_new[:, lanes], axis=1, keepdims=True))
        total = o_ref[h, pl.ds(h, rows, stride=SUB), :]
        total = total + own.astype(BF16).astype(F32) * value_new[:, lanes]
        den = d_ref[pl.ds(h, rows, stride=SUB), :] + own
        pieces.append((total / den).astype(BF16))
    attended = jnp.concatenate(pieces, axis=1)

    def pair_copy(m):
        return remote(
            part_ref.at[1 - c, m], pair_ref.at[m], pair_send.at[m], pair_recv.at[m], partner
        )

    def rs_copy(m):
        return remote(
            ps_ref.at[m], rs_ref.at[m0], rs_send.at[m], rs_recv.at[m0], (s + 1, 2 * m + c)
        )

    def frs_copy(j, m):
        return remote(
            fps_ref.at[j, m],
            frs_ref.at[m0],
            frs_send.at[j, m],
            frs_recv.at[m0],
            (jnp.int32(j), 2 * m + c),
        )

    wo_copy.wait()
    for m in range(chips):
        both = jnp.dot(
            attended,
            wo_ref[:, 2 * m * feats : 2 * (m + 1) * feats],
            preferred_element_type=F32,
        ).astype(BF16)
        part_ref[0, m] = both[:, :feats]
        part_ref[1, m] = both[:, feats:]
        pair_copy(m).start()

    out_rows = out_ref.shape[0]

    def pair_sum(m):
        pair_copy(m).wait_recv()
        return part_ref[c, m].astype(F32) + pair_ref[m].astype(F32)

    @pl.when(s < last)
    def _():
        for m in range(chips):
            ps_ref[m] = pair_sum(m).astype(BF16)
            rs_copy(m).start()

    @pl.when(s == last)
    def _():
        for m in range(chips):
            total = pair_sum(m)
            for j in range(sections):
                fps_ref[j, m] = total[j * out_rows : (j + 1) * out_rows].astype(BF16)
                if j < last:
                    frs_copy(j, m).start()
                else:

                    @pl.when(m0 != m)
                    def _():
                        frs_copy(j, m).start()

    base = emb_ref[...].astype(F32)
    mix_ref[...] = coef(sections, 0) * base
    avl_ref[...] = coef(last, 0) * base

    def mix_in(level, value):
        value = value.astype(F32)
        mix_ref[...] = mix_ref[...] + coef(sections, level) * value
        avl_ref[...] = avl_ref[...] + coef(last, level) * value

    def mix_before(level, carry):
        mix_in(level, g_ref[level, c, m0])
        return carry

    def mix_after(level, carry):
        landed(fin_ref.at[level], fin_recv.at[level])
        mix_in(level, fin_ref[level])
        return carry

    lax.fori_loop(1, s + 1, mix_before, 0)
    lax.fori_loop(s + 1, sections, mix_after, 0)

    @pl.when(s == last)
    def _():
        frs_ref[m0] = fps_ref[last, m0]

    top_out = coef(sections, sections)
    for k in range(chips):
        m = lax.rem(m0 + k, chips)
        if k == 0:

            @pl.when(s < last)
            def _():
                landed(frs_ref.at[m], frs_recv.at[m])

            summed = frs_ref[m].astype(F32)
        else:
            landed(frs_ref.at[m], frs_recv.at[m])
            summed = summed + frs_ref[m].astype(F32)
    for j in range(sections):

        @pl.when(s == j)
        def _():
            mine = slice(j * out_rows, (j + 1) * out_rows)
            final = (avl_ref[mine, :].astype(BF16).astype(F32) + summed).astype(BF16)
            out_ref[...] = (mix_ref[mine, :] + top_out * final.astype(F32)).astype(BF16)

    for k in range(1, chips):
        spread(outb_ref, s, 1, lax.rem(m0 + k, chips)).wait_send()
    for m in range(chips):
        pair_copy(m).wait_send()

    @pl.when(s > 0)
    def _():
        for k in range(1, chips):
            spread(emb_ref, 0, 0, lax.rem(m0 + k, chips)).wait_send()

    @pl.when(s < last)
    def _():
        for m in range(chips):
            rs_copy(m).wait_send()

    @pl.when(s == last)
    def _():
        for m in range(chips):
            for j in range(sections):
                if j < last:
                    frs_copy(j, m).wait_send()
                else:

                    @pl.when(m0 != m)
                    def _():
                        frs_copy(j, m).wait_send()

    def drain_forward(level, carry):
        for m in range(chips):
            forward(emb_ref, level, m).wait_send()
        return carry

    def drain_later(j, carry):
        for m in range(chips):
            to_later(j, m).wait_send()
        return carry

    def drain_earlier(j, carry):
        to_earlier(j).wait_send()
        return carry

    lax.fori_loop(0, s + 1, drain_forward, 0)

    @pl.when(s > 0)
    def _():
        lax.fori_loop(s + 1, sections, drain_later, 0)
        lax.fori_loop(0, s, drain_earlier, 0)


def per_device(sections, tensors, emb, gain, qkv, wo, ck, cv, dw, ds, order, lengths):
    rows, feats = emb.shape
    chips = tensors // 2
    w = jnp.transpose(qkv, (0, 2, 1, 3))[0].reshape(3, chips, 2 * feats, -1)
    width = w.shape[-1]
    cache = ck.shape[2]
    vmem = pl.BlockSpec(memory_space=pltpu.VMEM)
    smem = pl.BlockSpec(memory_space=pltpu.SMEM)
    hbm = pl.BlockSpec(memory_space=pl.ANY)
    dma = pltpu.SemaphoreType.DMA
    return pl.pallas_call(
        functools.partial(kernel, sections, tensors),
        out_shape=jax.ShapeDtypeStruct((rows // sections, feats), BF16),
        in_specs=[vmem, vmem, hbm, hbm, hbm, hbm, smem, smem, smem, smem],
        out_specs=vmem,
        scratch_shapes=[
            pltpu.VMEM(w.shape, BF16),
            pltpu.VMEM(wo.shape[1:], BF16),
            pltpu.VMEM(ck.shape[1:], BF16),
            pltpu.VMEM(cv.shape[1:], BF16),
            pltpu.VMEM((sections, 2, chips, rows, feats), BF16),
            pltpu.VMEM((sections, rows, feats), BF16),
            pltpu.VMEM((2, chips, rows, feats), F32),
            pltpu.VMEM((chips, rows, 2 * feats), BF16),
            pltpu.VMEM((rows, width), F32),
            pltpu.VMEM((rows * SUB, cache), F32),
            pltpu.VMEM((rows, SUB, cache), BF16),
            pltpu.VMEM((rows * SUB, HD), F32),
            pltpu.VMEM((width // HD, rows * SUB, HD), F32),
            pltpu.VMEM((2, chips, rows, feats), BF16),
            pltpu.VMEM((chips, rows, feats), BF16),
            pltpu.VMEM((chips, rows, feats), BF16),
            pltpu.VMEM((chips, rows, feats), BF16),
            pltpu.VMEM((sections, chips, rows // sections, feats), BF16),
            pltpu.VMEM((chips, rows // sections, feats), BF16),
            pltpu.VMEM((rows, feats), BF16),
            pltpu.VMEM((rows, feats), F32),
            pltpu.VMEM((rows, feats), F32),
            dma((6,)),
            dma((sections, 2, chips)),
            dma((2, chips)),
            dma((sections, chips)),
            dma((chips,)),
            dma((chips,)),
            dma((chips,)),
            dma((chips,)),
            dma((sections, chips)),
            dma((chips,)),
            dma((sections, chips)),
            dma((sections,)),
            dma((sections,)),
            pltpu.SemaphoreType.REGULAR,
        ],
        compiler_params=pltpu.CompilerParams(
            collective_id=0, has_side_effects=True, vmem_limit_bytes=56 * 1024 * 1024
        ),
    )(emb, gain, w, wo[0], ck[0], cv[0], dw, ds, order, lengths)


def solution(mesh):
    placed = (
        P(None, "tensor"),
        P("section", None),
        P("section", None, None, "tensor"),
        P("section", "tensor", None),
        P("section", None, None, "tensor"),
        P("section", None, None, "tensor"),
        P(),
        P(),
        P(),
        P(),
    )
    return jax.shard_map(
        functools.partial(per_device, mesh.shape["section"], mesh.shape["tensor"]),
        mesh=mesh,
        in_specs=placed,
        out_specs=P("section", "tensor"),
        check_vma=False,
    )
```

```python
import functools

import jax
import jax.numpy as jnp
from jax import lax
from jax.experimental import pallas as pl
from jax.experimental.pallas import tpu as pltpu
from jax.sharding import PartitionSpec as P

HD = 128
SUB = 8
MESH = pl.DeviceIdType.MESH
F32 = jnp.float32
BF16 = jnp.bfloat16


def kernel(
    sections,
    tensors,
    emb_ref,
    gain_ref,
    w_hbm,
    wo_hbm,
    k_hbm,
    v_hbm,
    dw_ref,
    ds_ref,
    order_ref,
    len_ref,
    out_ref,
    w_ref,
    wo_ref,
    k_ref,
    v_ref,
    g_ref,
    fin_ref,
    acc_ref,
    x_ref,
    q_ref,
    s_ref,
    p_ref,
    d_ref,
    o_ref,
    part_ref,
    pair_ref,
    ps_ref,
    rs_ref,
    fps_ref,
    frs_ref,
    outb_ref,
    mix_ref,
    avl_ref,
    loc_sem,
    g_recv,
    g_send,
    fwd_send,
    pair_send,
    pair_recv,
    rs_send,
    rs_recv,
    frs_send,
    frs_recv,
    bc_send,
    fin_send,
    fin_recv,
    ready_sem,
):
    chips = tensors // 2
    last = sections - 1
    s = lax.axis_index("section")
    t = lax.axis_index("tensor")
    c = lax.rem(t, 2)
    m0 = t // 2
    partner = (s, t + 1 - 2 * c)
    rows, feats = emb_ref.shape
    slots = dw_ref.shape[1]
    width = w_ref.shape[3]
    heads = width // HD

    def coef(i, j):
        total = jnp.float32(0.0)
        for k in range(slots):
            total = total + jnp.where(ds_ref[i, k] == j, dw_ref[i, k], jnp.float32(0.0))
        return total

    def remote(src, dst, send, recv, device):
        return pltpu.make_async_remote_copy(
            src_ref=src,
            dst_ref=dst,
            send_sem=send,
            recv_sem=recv,
            device_id=device,
            device_id_type=MESH,
        )

    def landed(ref, sem):
        pltpu.make_async_copy(ref, ref, sem).wait()

    barrier = pltpu.get_barrier_semaphore()
    pl.semaphore_signal(barrier, inc=1, device_id=partner, device_id_type=MESH)
    for k in range(1, chips):
        m = lax.rem(m0 + k, chips)
        pl.semaphore_signal(barrier, inc=1, device_id=(s, 2 * m + c), device_id_type=MESH)
    for k in range(1, sections):
        j = lax.rem(s + k, sections)
        pl.semaphore_signal(barrier, inc=1, device_id=(j, t), device_id_type=MESH)

    w_copies = [
        pltpu.make_async_copy(w_hbm.at[j], w_ref.at[j], loc_sem.at[j]) for j in range(3)
    ]
    k_copy = pltpu.make_async_copy(k_hbm, k_ref, loc_sem.at[3])
    v_copy = pltpu.make_async_copy(v_hbm, v_ref, loc_sem.at[4])
    wo_copy = pltpu.make_async_copy(wo_hbm, wo_ref, loc_sem.at[5])
    for cp in w_copies + [k_copy, v_copy, wo_copy]:
        cp.start()
    acc_ref[...] = jnp.zeros_like(acc_ref)

    pl.semaphore_wait(barrier, chips + sections - 1)
    for k in range(1, sections):
        j = lax.rem(s + k, sections)
        pl.semaphore_signal(ready_sem, inc=1, device_id=(j, t), device_id_type=MESH)

    def spread(src, level, group, m):
        return remote(
            src,
            g_ref.at[level, c, m0],
            g_send.at[group, m],
            g_recv.at[level, c, m0],
            (s, 2 * m + c),
        )

    def forward(src, level, m):
        return remote(
            src, g_ref.at[level, c, m], fwd_send.at[level, m], g_recv.at[level, c, m], partner
        )

    def arrive(level, parity, m):
        landed(g_ref.at[level, parity, m], g_recv.at[level, parity, m])

    def spread_start(src, level, group):
        for k in range(1, chips):
            spread(src, level, group, lax.rem(m0 + k, chips)).start()
        forward(src, level, m0).start()
        g_ref[level, c, m0] = src[...]

    def to_later(j, m):
        return remote(
            outb_ref,
            g_ref.at[s, c, m0],
            bc_send.at[j, m],
            g_recv.at[s, c, m0],
            (j, 2 * m + c),
        )

    def to_earlier(j):
        return remote(outb_ref, fin_ref.at[s], fin_send.at[j], fin_recv.at[s], (j, t))

    @pl.when(s == 0)
    def _():
        outb_ref[...] = emb_ref[...]

    @pl.when(s > 0)
    def _():
        spread_start(emb_ref, 0, 0)

        def add_level(level, carry):
            for k in range(chips):
                m = lax.rem(m0 + k, chips)
                if k == 0:

                    @pl.when(level > 0)
                    def _():
                        arrive(level, c, m)
                        forward(g_ref.at[level, c, m], level, m).start()
                else:
                    arrive(level, c, m)
                    forward(g_ref.at[level, c, m], level, m).start()
            for m in range(chips):
                arrive(level, 1 - c, m)
            cl = coef(s, level)
            for m in range(chips):
                for par in range(2):
                    acc_ref[par, m] = acc_ref[par, m] + cl * g_ref[level, par, m].astype(F32)
            return carry

        lax.fori_loop(0, s, add_level, 0)

        mix_ref[...] = jnp.zeros_like(mix_ref)

        def add_below(level, carry):
            mix_ref[...] = mix_ref[...] + coef(s - 1, level) * g_ref[level, c, m0].astype(F32)
            return carry

        lax.fori_loop(0, s, add_below, 0)
        produced = mix_ref[...].astype(BF16).astype(F32)
        for k in range(chips):
            m = lax.rem(m0 + k, chips)
            landed(rs_ref.at[m], rs_recv.at[m])
            produced = produced + rs_ref[m].astype(F32)
        outb_ref[...] = produced.astype(BF16)

    spread_start(outb_ref, s, 1)
    pl.semaphore_wait(ready_sem, sections - 1)

    @pl.when(s > 0)
    def _():
        def send_later(j, carry):
            for m in range(chips):
                to_later(j, m).start()
            return carry

        def send_earlier(j, carry):
            to_earlier(j).start()
            return carry

        lax.fori_loop(s + 1, sections, send_later, 0)
        lax.fori_loop(0, s, send_earlier, 0)

    top = coef(s, s)
    squares = jnp.zeros((rows, 1), F32)
    proj = [jnp.zeros((rows, width), F32) for _ in range(3)]
    lag = chips
    for k in range(chips + lag):
        if 0 < k < chips:
            m = lax.rem(m0 + k, chips)
            arrive(s, c, m)
            forward(g_ref.at[s, c, m], s, m).start()
        k = k - lag
        if k < 0:
            continue
        m = lax.rem(m0 + k, chips)
        arrive(s, 1 - c, m)
        gains = gain_ref[:, pl.ds(pl.multiple_of(m * 2 * feats, HD), 2 * feats)]
        for par in range(2):
            cols = slice(par * feats, (par + 1) * feats)
            avg = acc_ref[par, m] + top * g_ref[s, par, m].astype(F32)
            avg = avg.astype(BF16).astype(F32)
            squares = squares + jnp.sum(avg * avg, axis=1, keepdims=True)
            x_ref[k, :, cols] = (avg * gains[:, cols]).astype(BF16)
        if k == 0:
            for cp in w_copies:
                cp.wait()
        x = x_ref[k]
        for j in range(3):
            proj[j] = proj[j] + jnp.dot(x, w_ref[j, m], preferred_element_type=F32)
    inv_rms = lax.rsqrt(squares / (tensors * feats) + 1e-05)
    query = (proj[0] * inv_rms * HD ** (-0.5)).astype(BF16).astype(F32)
    q_ref[...] = query
    key_new = (proj[1] * inv_rms).astype(BF16).astype(F32)
    value_new = (proj[2] * inv_rms).astype(BF16).astype(F32)

    cache = k_ref.shape[1]
    head_of_lane = lax.broadcasted_iota(jnp.int32, (SUB, width), 1) // HD
    head_rows = lax.broadcasted_iota(jnp.int32, (SUB, width), 0)
    head_mask = head_of_lane == head_rows
    position = lax.broadcasted_iota(jnp.int32, (SUB, cache), 1)
    group = rows

    k_copy.wait()

    def score_step(step, carry):
        for u in range(group):
            b = step * group + u
            row = order_ref[b]
            qb = jnp.broadcast_to(q_ref[pl.ds(b, 1), :], (SUB, width))
            qb = jnp.where(head_mask, qb, 0.0).astype(BF16)
            sc = lax.dot_general(
                qb, k_ref[row], (((1,), (1,)), ((), ())), preferred_element_type=F32
            )
            s_ref[pl.ds(pl.multiple_of(b * SUB, SUB), SUB), :] = jnp.where(
                position < len_ref[b], sc, -1e30
            )
        return carry

    lax.fori_loop(0, rows // group, score_step, 0)
    p = jnp.exp(s_ref[...])
    d_ref[...] = jnp.broadcast_to(jnp.sum(p, axis=1, keepdims=True), (rows * SUB, HD))
    p_ref[...] = p.astype(BF16).reshape(rows, SUB, cache)

    v_copy.wait()

    def value_step(step, carry):
        for u in range(group):
            b = step * group + u
            row = order_ref[b]
            pv = jnp.dot(p_ref[b], v_ref[row], preferred_element_type=F32)
            for h in range(heads):
                o_ref[h, pl.ds(pl.multiple_of(b * SUB, SUB), SUB), :] = pv[
                    :, h * HD : (h + 1) * HD
                ]
        return carry

    lax.fori_loop(0, rows // group, value_step, 0)

    pieces = []
    for h in range(heads):
        lanes = slice(h * HD, (h + 1) * HD)
        own = jnp.exp(jnp.sum(query[:, lanes] * key_new[:, lanes], axis=1, keepdims=True))
        total = o_ref[h, pl.ds(h, rows, stride=SUB), :]
        total = total + own.astype(BF16).astype(F32) * value_new[:, lanes]
        den = d_ref[pl.ds(h, rows, stride=SUB), :] + own
        pieces.append((total / den).astype(BF16))
    attended = jnp.concatenate(pieces, axis=1)

    def pair_copy(m):
        return remote(
            part_ref.at[1 - c, m], pair_ref.at[m], pair_send.at[m], pair_recv.at[m], partner
        )

    def rs_copy(m):
        return remote(
            ps_ref.at[m], rs_ref.at[m0], rs_send.at[m], rs_recv.at[m0], (s + 1, 2 * m + c)
        )

    def frs_copy(j, m):
        return remote(
            fps_ref.at[j, m],
            frs_ref.at[m0],
            frs_send.at[j, m],
            frs_recv.at[m0],
            (jnp.int32(j), 2 * m + c),
        )

    wo_copy.wait()
    for m in range(chips):
        both = jnp.dot(
            attended,
            wo_ref[:, 2 * m * feats : 2 * (m + 1) * feats],
            preferred_element_type=F32,
        ).astype(BF16)
        part_ref[0, m] = both[:, :feats]
        part_ref[1, m] = both[:, feats:]
        if m % 4 == 3:
            for i in range(m - 3, m + 1):
                pair_copy(i).start()

    out_rows = out_ref.shape[0]

    def pair_sum(m):
        pair_copy(m).wait_recv()
        return part_ref[c, m].astype(F32) + pair_ref[m].astype(F32)

    @pl.when(s < last)
    def _():
        for m in range(chips):
            ps_ref[m] = pair_sum(m).astype(BF16)
            rs_copy(m).start()

    @pl.when(s == last)
    def _():
        for m in range(chips):
            total = pair_sum(m)
            for j in range(sections):
                fps_ref[j, m] = total[j * out_rows : (j + 1) * out_rows].astype(BF16)
                if j < last:
                    frs_copy(j, m).start()
                else:

                    @pl.when(m0 != m)
                    def _():
                        frs_copy(j, m).start()

    base = emb_ref[...].astype(F32)
    mix_ref[...] = coef(sections, 0) * base
    avl_ref[...] = coef(last, 0) * base

    def mix_in(level, value):
        value = value.astype(F32)
        mix_ref[...] = mix_ref[...] + coef(sections, level) * value
        avl_ref[...] = avl_ref[...] + coef(last, level) * value

    def mix_before(level, carry):
        mix_in(level, g_ref[level, c, m0])
        return carry

    def mix_after(level, carry):
        landed(fin_ref.at[level], fin_recv.at[level])
        mix_in(level, fin_ref[level])
        return carry

    lax.fori_loop(1, s + 1, mix_before, 0)
    lax.fori_loop(s + 1, sections, mix_after, 0)

    @pl.when(s == last)
    def _():
        frs_ref[m0] = fps_ref[last, m0]

    top_out = coef(sections, sections)
    for k in range(chips):
        m = lax.rem(m0 + k, chips)
        if k == 0:

            @pl.when(s < last)
            def _():
                landed(frs_ref.at[m], frs_recv.at[m])

            summed = frs_ref[m].astype(F32)
        else:
            landed(frs_ref.at[m], frs_recv.at[m])
            summed = summed + frs_ref[m].astype(F32)
    for j in range(sections):

        @pl.when(s == j)
        def _():
            mine = slice(j * out_rows, (j + 1) * out_rows)
            final = (avl_ref[mine, :].astype(BF16).astype(F32) + summed).astype(BF16)
            out_ref[...] = (mix_ref[mine, :] + top_out * final.astype(F32)).astype(BF16)

    for k in range(1, chips):
        spread(outb_ref, s, 1, lax.rem(m0 + k, chips)).wait_send()
    for m in range(chips):
        pair_copy(m).wait_send()

    @pl.when(s > 0)
    def _():
        for k in range(1, chips):
            spread(emb_ref, 0, 0, lax.rem(m0 + k, chips)).wait_send()

    @pl.when(s < last)
    def _():
        for m in range(chips):
            rs_copy(m).wait_send()

    @pl.when(s == last)
    def _():
        for m in range(chips):
            for j in range(sections):
                if j < last:
                    frs_copy(j, m).wait_send()
                else:

                    @pl.when(m0 != m)
                    def _():
                        frs_copy(j, m).wait_send()

    def drain_forward(level, carry):
        for m in range(chips):
            forward(emb_ref, level, m).wait_send()
        return carry

    def drain_later(j, carry):
        for m in range(chips):
            to_later(j, m).wait_send()
        return carry

    def drain_earlier(j, carry):
        to_earlier(j).wait_send()
        return carry

    lax.fori_loop(0, s + 1, drain_forward, 0)

    @pl.when(s > 0)
    def _():
        lax.fori_loop(s + 1, sections, drain_later, 0)
        lax.fori_loop(0, s, drain_earlier, 0)


def per_device(sections, tensors, emb, gain, qkv, wo, ck, cv, dw, ds, order, lengths):
    rows, feats = emb.shape
    chips = tensors // 2
    w = jnp.transpose(qkv, (0, 2, 1, 3))[0].reshape(3, chips, 2 * feats, -1)
    width = w.shape[-1]
    cache = ck.shape[2]
    vmem = pl.BlockSpec(memory_space=pltpu.VMEM)
    smem = pl.BlockSpec(memory_space=pltpu.SMEM)
    hbm = pl.BlockSpec(memory_space=pl.ANY)
    dma = pltpu.SemaphoreType.DMA
    return pl.pallas_call(
        functools.partial(kernel, sections, tensors),
        out_shape=jax.ShapeDtypeStruct((rows // sections, feats), BF16),
        in_specs=[vmem, vmem, hbm, hbm, hbm, hbm, smem, smem, smem, smem],
        out_specs=vmem,
        scratch_shapes=[
            pltpu.VMEM(w.shape, BF16),
            pltpu.VMEM(wo.shape[1:], BF16),
            pltpu.VMEM(ck.shape[1:], BF16),
            pltpu.VMEM(cv.shape[1:], BF16),
            pltpu.VMEM((sections, 2, chips, rows, feats), BF16),
            pltpu.VMEM((sections, rows, feats), BF16),
            pltpu.VMEM((2, chips, rows, feats), F32),
            pltpu.VMEM((chips, rows, 2 * feats), BF16),
            pltpu.VMEM((rows, width), F32),
            pltpu.VMEM((rows * SUB, cache), F32),
            pltpu.VMEM((rows, SUB, cache), BF16),
            pltpu.VMEM((rows * SUB, HD), F32),
            pltpu.VMEM((width // HD, rows * SUB, HD), F32),
            pltpu.VMEM((2, chips, rows, feats), BF16),
            pltpu.VMEM((chips, rows, feats), BF16),
            pltpu.VMEM((chips, rows, feats), BF16),
            pltpu.VMEM((chips, rows, feats), BF16),
            pltpu.VMEM((sections, chips, rows // sections, feats), BF16),
            pltpu.VMEM((chips, rows // sections, feats), BF16),
            pltpu.VMEM((rows, feats), BF16),
            pltpu.VMEM((rows, feats), F32),
            pltpu.VMEM((rows, feats), F32),
            dma((6,)),
            dma((sections, 2, chips)),
            dma((2, chips)),
            dma((sections, chips)),
            dma((chips,)),
            dma((chips,)),
            dma((chips,)),
            dma((chips,)),
            dma((sections, chips)),
            dma((chips,)),
            dma((sections, chips)),
            dma((sections,)),
            dma((sections,)),
            pltpu.SemaphoreType.REGULAR,
        ],
        compiler_params=pltpu.CompilerParams(
            collective_id=0, has_side_effects=True, vmem_limit_bytes=56 * 1024 * 1024
        ),
    )(emb, gain, w, wo[0], ck[0], cv[0], dw, ds, order, lengths)


def solution(mesh):
    placed = (
        P(None, "tensor"),
        P("section", None),
        P("section", None, None, "tensor"),
        P("section", "tensor", None),
        P("section", None, None, "tensor"),
        P("section", None, None, "tensor"),
        P(),
        P(),
        P(),
        P(),
    )
    return jax.shard_map(
        functools.partial(per_device, mesh.shape["section"], mesh.shape["tensor"]),
        mesh=mesh,
        in_specs=placed,
        out_specs=P("section", "tensor"),
        check_vma=False,
    )
```
